256 devices in a mesh: dp: 4 (over y), expert: 32 (over z, x), tensor: 2 (over core).
Axes of the slice: x: 4, y: 4, z: 8, core: 2. Of those that a mesh axis runs over, the one named last changes fastest.
Arguments:
- tokens: bfloat16 [1, 2048, 3584], P(None, ('dp', 'expert'), 'tensor'), may hold values from -6 to 6
- gate_weight: bfloat16 [128, 3584, 1024], P(('dp', 'expert'), None, 'tensor'), may hold values from -0.09375 to 0.09375
- up_weight: bfloat16 [128, 3584, 1024], P(('dp', 'expert'), None, 'tensor'), may hold values from -0.09375 to 0.09375
- down_weight: bfloat16 [128, 1024, 3584], P(('dp', 'expert'), 'tensor'), may hold values from -0.1875 to 0.1875
- expert_ids: int32 [1, 2048, 8], P(None, ('dp', 'expert')), may hold values from 0 to 127, all different within a row; in each aligned block of 16 rows (0 to 15, 16 to 31, ..., all dimensions but the last counted through in order) at most 2 rows name the same one
- gate_codes: int32 [1, 2048, 8], P(None, ('dp', 'expert')), may hold values from 1 to 32767
Outputs:
- mixed: bfloat16 [1, 2048, 3584], P(None, ('dp', 'expert'), 'tensor')
The draws below stay inside these ranges and needn't reach their ends.
Inputs may be any that keep to these rules, and one draw needn't show every extreme that they name: `expert_ids`: the 8 experts of one token differ. For every step, of the 16 tokens that one index of dp+expert holds, no expert is named by more than 2.
All inputs are finite; a program needn't handle non-finite values.
Results may differ from the reference program's by a relative error of at most 0.0095.
Values may be sent and summed in bfloat16 or wider, within the bound.
A program may use at most 64 MiB of HBM per device.

```python
import math
import jax
import jax.numpy as jnp
import numpy as np
from jax import lax

D = 3584
FF = 1024
TOP = 8
STEPS = 1
TOK = 16
EXPERTS = 128
MOST = 2
TOKENS = 2048
N_DP = 4
N_EXPERT = 32
N_TENSOR = 2


def with_ends(array, own_key, smallest, high):
    place = [jax.random.randint(jax.random.fold_in(own_key, axis), (), 0, length) for axis, length in enumerate(array.shape)]
    main_axis = array.shape.index(max(array.shape))
    beside = place[:main_axis] + [(place[main_axis] + 1) % array.shape[main_axis]] + place[main_axis + 1:]
    return array.at[tuple(place)].set(smallest).at[tuple(beside)].set(high)


def steps_of(key, shape, shards, low, top_value):
    loudness, own = 1.0, jax.random.fold_in(key, 6)
    for position, parts in shards:
        draws = jnp.exp(jax.random.uniform(jax.random.fold_in(own, position), (parts,), jnp.float32, low / len(shards), top_value / len(shards)))
        loudness = loudness * jnp.repeat(draws, shape[position] // parts).reshape([-1 if axis == position else 1 for axis in range(len(shape))])
    return loudness


def shared_out(stream_key, own, number, rows, number_of, top, bound, skew):
    ranking = jax.random.permutation(stream_key, number_of)
    crowded, common = load_shares(number_of, rows * top, bound, skew, True), load_shares(number_of, rows * top, bound, skew, False)
    places = jnp.arange(number_of)

    def named(tallies, rotation):
        used = int((tallies > 0).sum())
        fixed = max(1, used // 4)
        moved = fixed + (places - fixed + rotation * (used - fixed)) % max(1, number_of - fixed)
        return jnp.zeros((number_of,), jnp.int32).at[ranking[jnp.where(places < fixed, places, moved)]].set(jnp.asarray(tallies, jnp.int32))

    tallies = jnp.where(number % 4 == 0, named(crowded, number // 4), named(common, number - number // 4 - 1))
    mixed = jax.random.permutation(jax.random.fold_in(own, 3), number_of)
    source_of, taker = mixed[0:number_of // 2 * 2:2], mixed[1:number_of // 2 * 2:2]
    margin = jnp.minimum(tallies[source_of] - 1, bound - tallies[taker]) // 2
    margin = jnp.where((source_of == ranking[0]) | (taker == ranking[0]) | (tallies[taker] == 0), 0, jnp.maximum(margin, 0))
    moved = jax.random.randint(jax.random.fold_in(own, 4), (number_of // 2,), 0, 1 << 20) % (margin + 1)
    tallies = tallies.at[source_of].add(-moved).at[taker].add(moved)
    members = jnp.searchsorted(jnp.cumsum(tallies), jnp.arange(rows * top), side="right").astype(jnp.int32)
    grid = members.reshape(top, rows).T
    grid = grid[jax.random.permutation(jax.random.fold_in(own, 1), rows)]
    rotation = jax.random.randint(jax.random.fold_in(own, 2), (rows, 1), 0, top)
    return jnp.take_along_axis(grid, (jnp.arange(top)[None, :] + rotation) % top, axis=1)


def load_shares(amount, total, bound, slope, full):
    weights = [(1 << 20) // math.isqrt(grade ** slope) + 1 for grade in range(1, amount + 1)]
    largest = bound if full else min(bound, max(-(-total // amount), total * weights[0] // sum(weights)))
    least = 1 if total - largest >= amount - 1 else 0
    given, spare = [largest] + [least] * (amount - 1), total - largest - least * (amount - 1)
    while spare > 0:
        free = [i for i in range(1, amount) if given[i] < largest] or [i for i in range(1, amount) if given[i] < bound]
        pool, left = sum([weights[i] for i in free]), spare
        for i in free:
            extra = min(bound - given[i], max(1, left * weights[i] // pool), spare)
            given[i] = given[i] + extra
            spare = spare - extra
    return np.array(given)


def noise(own_key, extent, spread, bound, shards=(), kind=jnp.bfloat16):
    level = steps_of(own_key, extent, shards, -0.22, 0.18) if shards else 1.0
    values = jax.random.normal(own_key, extent, jnp.float32) * spread * level
    return jnp.minimum(jnp.maximum(values, -bound), bound).astype(kind)


def setup_inputs(seed: int = 0) -> dict:
    keys = jax.random.split(jax.random.key(seed), 7)
    tokens = noise(keys[0], (STEPS, TOKENS, D), 1.0, 6.0, ((1, 128), (2, 2)))
    gate_weight = noise(keys[1], (EXPERTS, D, FF), D ** -0.5, 0.09375, ((0, 128), (2, 2)))
    up_weight = noise(keys[2], (EXPERTS, D, FF), D ** -0.5, 0.09375, ((0, 128), (2, 2)))
    down_weight = noise(keys[3], (EXPERTS, FF, D), FF ** -0.5, 0.1875, ((0, 128), (1, 2)))
    expert_ids_keys = jax.random.split(jax.random.fold_in(keys[4], 1), STEPS * TOKENS // TOK)
    expert_ids_turns = jax.random.permutation(jax.random.fold_in(keys[4], 3), STEPS * TOKENS // TOK)
    expert_ids = jax.vmap(lambda own, number: shared_out(jax.random.fold_in(keys[4], 2), own, number, TOK, EXPERTS, TOP, MOST, 2))(expert_ids_keys, expert_ids_turns).reshape((STEPS, TOKENS, TOP))
    gate_codes = with_ends(jax.random.randint(keys[5], (STEPS, TOKENS, TOP), 1, 32768), jax.random.fold_in(keys[5], 1), 1, 32767).astype(jnp.int32)
    return {"tokens": tokens, "gate_weight": gate_weight, "up_weight": up_weight, "down_weight": down_weight, "expert_ids": expert_ids, "gate_codes": gate_codes}


def reference(tokens, gate_weight, up_weight, down_weight, expert_ids, gate_codes):
    pair_count = STEPS * TOKENS * TOP
    flat_tokens = tokens.reshape(STEPS * TOKENS, D)
    flat_ids = expert_ids.reshape(pair_count).astype(jnp.int32)
    codes = gate_codes.astype(jnp.float32)
    shares = (codes / jnp.sum(codes, axis=2, keepdims=True)).reshape(pair_count)
    capacity = STEPS * N_DP * N_EXPERT * MOST
    half_units = FF // N_TENSOR

    def one_expert(expert, total):
        chosen = jnp.nonzero(flat_ids == expert, size=capacity, fill_value=pair_count)[0].astype(jnp.int32)
        valid = chosen < pair_count
        clipped = jnp.minimum(chosen, pair_count - 1).astype(jnp.int32)
        token_rows = (clipped // TOP).astype(jnp.int32)
        inputs = flat_tokens[token_rows]
        w_gate = lax.dynamic_index_in_dim(gate_weight, expert, 0, keepdims=False)
        w_up = lax.dynamic_index_in_dim(up_weight, expert, 0, keepdims=False)
        w_down = lax.dynamic_index_in_dim(down_weight, expert, 0, keepdims=False)
        gated = jnp.dot(inputs, w_gate, preferred_element_type=jnp.float32)
        lifted = jnp.dot(inputs, w_up, preferred_element_type=jnp.float32)
        hidden = (jax.nn.silu(gated) * lifted).astype(jnp.bfloat16)
        summed = jnp.zeros((capacity, D), jnp.float32)
        for group in range(N_TENSOR):
            piece = jnp.dot(hidden[:, group * half_units:(group + 1) * half_units],
                            w_down[group * half_units:(group + 1) * half_units],
                            preferred_element_type=jnp.float32)
            summed = summed + lax.optimization_barrier(piece.astype(jnp.bfloat16)).astype(jnp.float32)
        expert_out = lax.optimization_barrier(summed.astype(jnp.bfloat16)).astype(jnp.float32)
        scale = jnp.where(valid, shares[clipped], jnp.zeros((capacity,), jnp.float32))
        return total.at[token_rows].add(scale[:, None] * expert_out)

    total = lax.fori_loop(0, N_DP * N_EXPERT, one_expert, jnp.zeros((STEPS * TOKENS, D), jnp.float32))
    return total.astype(jnp.bfloat16).reshape(STEPS, TOKENS, D)
```

```python
import jax
import jax.numpy as jnp
from jax import lax
from jax.experimental import pallas as pl
from jax.experimental.pallas import tpu as pltpu
from jax.sharding import PartitionSpec as P

MESH = pl.DeviceIdType.MESH
BF = jnp.bfloat16
F32 = jnp.float32
NX, NY, NZ = 4, 4, 8
TOK, TOP, SLOTS = 16, 8, 2
PLANE = NX * NY
META = 128
GROUPS = ((0, 1, 7, 2), (6, 3, 5, 4))
PER = len(GROUPS[0])
BLOCK = PER * SLOTS
ROWS = PLANE * BLOCK
SENDS = ((1, 0), (3, 0), (0, 1), (0, 3), (1, 1), (3, 3), (1, 3), (3, 1), (2, 0), (0, 2), (2, 1), (1, 2), (2, 3), (3, 2), (2, 2))


def kernel(tok_hbm, ids_hbm, codes_hbm, wg_hbm, wu_hbm, wd_hbm, out_ref,
           held, ids_v, codes_v, meta, packed, own, par, wg, wu, wd, mine, theirs, back, came, sums,
           in_sem, w_sem, zs_sem, zr_sem, ds_sem, dr_sem, fs_sem, fr_sem, ps_sem, pr_sem, bs_sem, br_sem, os_sem, or_sem):
    y = lax.axis_index("dp")
    e = lax.axis_index("expert")
    c = lax.axis_index("tensor")
    x = lax.rem(e, NX)
    z = e // NX
    half = own.shape[2]

    def at(dx, dy, dz):
        return (lax.rem(y + dy, NY), lax.rem(z + dz, NZ) * NX + lax.rem(x + dx, NX), c)

    partner = (y, e, 1 - c)
    near = pl.multiple_of(c * half, 128)
    far = pl.multiple_of((1 - c) * half, 128)

    def remote(src, dst, ss, rs, device):
        return pltpu.make_async_remote_copy(
            src_ref=src, dst_ref=dst, send_sem=ss, recv_sem=rs, device_id=device, device_id_type=MESH)

    first = [
        pltpu.make_async_copy(ids_hbm, ids_v, in_sem.at[0]),
        pltpu.make_async_copy(codes_hbm, codes_v, in_sem.at[1]),
        pltpu.make_async_copy(tok_hbm, held.at[0, :, pl.ds(0, half)], in_sem.at[2]),
    ]
    for copy in first:
        copy.start()
    barrier = pltpu.get_barrier_semaphore()
    for dz in range(1, NZ):
        pl.semaphore_signal(barrier, inc=1, device_id=at(0, 0, dz), device_id_type=MESH)
    for dx, dy in SENDS:
        pl.semaphore_signal(barrier, inc=1, device_id=at(dx, dy, 0), device_id_type=MESH)
    pl.semaphore_signal(barrier, inc=1, device_id=partner, device_id_type=MESH)
    weights = [
        pltpu.make_async_copy(wg_hbm.at[pl.ds(near, half)], wg.at[0], w_sem.at[0]),
        pltpu.make_async_copy(wu_hbm.at[pl.ds(near, half)], wu.at[0], w_sem.at[1]),
        pltpu.make_async_copy(wg_hbm.at[pl.ds(far, half)], wg.at[1], w_sem.at[2]),
        pltpu.make_async_copy(wu_hbm.at[pl.ds(far, half)], wu.at[1], w_sem.at[3]),
        pltpu.make_async_copy(wd_hbm.at[:, pl.ds(far, half)], wd.at[1], w_sem.at[4]),
        pltpu.make_async_copy(wd_hbm.at[:, pl.ds(near, half)], wd.at[0], w_sem.at[5]),
    ]
    for copy in weights:
        copy.start()

    first[0].wait()
    first[1].wait()
    meta[...] = jnp.zeros_like(meta)
    codes = codes_v[...]
    high = codes // 256
    meta[0:TOP, 0:TOK] = ids_v[...].astype(F32)
    meta[TOP:2 * TOP, 0:TOK] = high.astype(F32)
    meta[2 * TOP:3 * TOP, 0:TOK] = (codes - high * 256).astype(F32)
    held[0, :, half:half + META] = jnp.transpose(meta[...])[0:TOK].astype(BF)
    first[2].wait()
    pl.semaphore_wait(barrier, PLANE + NZ - 1)

    order = [dz for group in GROUPS for dz in group]
    z_copies = []
    for p, dz in enumerate(order):
        if dz:
            copy = remote(held.at[0], held.at[p], zs_sem.at[p], zr_sem.at[p], at(0, 0, dz))
            copy.start()
            z_copies.append(copy)
        else:
            z_copies.append(None)

    tokens = PER * TOK
    lane = lax.broadcasted_iota(jnp.int32, (1, ROWS), 1)
    offset = lane // BLOCK
    slot = lax.rem(lane, BLOCK)
    slot_source = slot // SLOTS
    slot_rank = lax.rem(slot, SLOTS).astype(F32)
    slot_expert = (lax.rem(y + offset // NX, NY) * (NX * NZ) + z * NX + lax.rem(x + lax.rem(offset, NX), NX)).astype(F32)
    row = lax.broadcasted_iota(jnp.int32, (tokens, 1), 0)
    same_source = (row // TOK) == slot_source
    r_i = lax.broadcasted_iota(jnp.int32, (tokens, tokens), 0)
    c_i = lax.broadcasted_iota(jnp.int32, (tokens, tokens), 1)
    earlier = jnp.where((r_i // TOK == c_i // TOK) & (c_i < r_i), 1.0, 0.0).astype(BF)

    def routes(g):
        m = held[PER * g:PER * (g + 1), :, half:half + META].reshape(tokens, META).astype(F32)
        number = m[:, TOP:2 * TOP] * 256.0 + m[:, 2 * TOP:3 * TOP]
        share = number / jnp.sum(number, axis=1, keepdims=True)
        hit = jnp.zeros((tokens, ROWS), F32)
        gate = jnp.zeros((tokens, ROWS), F32)
        for k in range(TOP):
            chosen = m[:, k:k + 1] == slot_expert
            hit = jnp.where(chosen, 1.0, hit)
            gate = jnp.where(chosen, share[:, k:k + 1], gate)
        rank = jnp.dot(earlier, hit.astype(BF), preferred_element_type=F32)
        take = (hit > 0.5) & same_source & (rank == slot_rank)
        return jnp.where(take, 1.0, 0.0), jnp.where(take, gate, 0.0)

    def block(dx, dy):
        return pl.ds((dy * NX + dx) * BLOCK, BLOCK)

    gates = []
    d_copies = []
    for g in range(len(GROUPS)):
        for p in range(PER * g, PER * (g + 1)):
            if z_copies[p] is not None:
                z_copies[p].wait_recv()
        take, gate = routes(g)
        gates.append(gate)
        rows = held[PER * g:PER * (g + 1), :, 0:half].reshape(tokens, half)
        packed[g] = jnp.dot(jnp.transpose(take).astype(BF), rows, preferred_element_type=F32).astype(BF)
        copies = []
        for i, (dx, dy) in enumerate(SENDS):
            copy = remote(packed.at[g, block(dx, dy)], own.at[g, block(dx, dy)], ds_sem.at[g, i], dr_sem.at[g, i], at(dx, dy, 0))
            copy.start()
            copies.append(copy)
        d_copies.append(copies)

    f_copies = []
    p_copies = []
    b_copies = []
    for g in range(len(GROUPS)):
        own[g, block(0, 0)] = packed[g, block(0, 0)]
        forwards = []
        for i, (dx, dy) in enumerate(((0, 0),) + SENDS):
            if i:
                d_copies[g][i - 1].wait_recv()
            copy = remote(own.at[g, block(dx, dy)], par.at[g, block(dx, dy)], fs_sem.at[g, i], fr_sem.at[g, i], partner)
            copy.start()
            forwards.append(copy)
        f_copies += forwards
        if g == 0:
            for copy in weights[:4]:
                copy.wait()
        rows = own[g]
        gated = jnp.dot(rows, wg[0], preferred_element_type=F32)
        lifted = jnp.dot(rows, wu[0], preferred_element_type=F32)
        for copy in forwards:
            copy.wait_recv()
        rows = par[g]
        gated += jnp.dot(rows, wg[1], preferred_element_type=F32)
        lifted += jnp.dot(rows, wu[1], preferred_element_type=F32)
        hidden = (gated / (1.0 + jnp.exp(-gated)) * lifted).astype(BF)
        if g == 0:
            for copy in weights[4:]:
                copy.wait()
        mine[g] = jnp.dot(hidden, wd[1], preferred_element_type=F32).astype(BF)
        copy = remote(mine.at[g], theirs.at[g], ps_sem.at[g], pr_sem.at[g], partner)
        copy.start()
        p_copies.append(copy)
        kept = jnp.dot(hidden, wd[0], preferred_element_type=F32).astype(BF).astype(F32)
        copy.wait_recv()
        back[g] = (kept + theirs[g].astype(F32)).astype(BF)
        copies = []
        for i, (dx, dy) in enumerate(SENDS):
            copy = remote(back.at[g, block(dx, dy)], came.at[g, block(dx, dy)], bs_sem.at[g, i], br_sem.at[g, i],
                          at(NX - dx, NY - dy, 0))
            copy.start()
            copies.append(copy)
        b_copies.append(copies)

    o_copies = []
    for g, group in enumerate(GROUPS):
        came[g, block(0, 0)] = back[g, block(0, 0)]
        for copy in b_copies[g]:
            copy.wait_recv()
        whole = gates[g].astype(BF)
        rest = (gates[g] - whole.astype(F32)).astype(BF)
        rows = came[g]
        total = jnp.dot(whole, rows, preferred_element_type=F32) + jnp.dot(rest, rows, preferred_element_type=F32)
        sums[PER * g:PER * (g + 1)] = total.astype(BF).reshape(PER, TOK, half)
        for q, dz in enumerate(group):
            p = PER * g + q
            if dz:
                copy = remote(sums.at[p], out_ref.at[p], os_sem.at[p], or_sem.at[p], at(0, 0, NZ - dz))
                copy.start()
                o_copies.append(copy)
            else:
                out_ref[p] = sums[p]
    for copy in o_copies:
        copy.wait()
    for copies in (z_copies, *d_copies, f_copies, p_copies, *b_copies):
        for copy in copies:
            if copy is not None:
                copy.wait_send()


def local(tokens, gate_weight, up_weight, down_weight, expert_ids, gate_codes):
    half = tokens.shape[2]
    full, units = gate_weight.shape[1], gate_weight.shape[2]
    groups = len(GROUPS)
    dma = pltpu.SemaphoreType.DMA
    n = len(SENDS)
    parts = pl.pallas_call(
        kernel,
        out_shape=jax.ShapeDtypeStruct((NZ, TOK, half), BF),
        in_specs=[pl.BlockSpec(memory_space=pl.ANY)] * 6,
        out_specs=pl.BlockSpec(memory_space=pltpu.VMEM),
        scratch_shapes=[
            pltpu.VMEM((NZ, TOK, half + META), BF),
            pltpu.VMEM((TOP, TOK), jnp.int32),
            pltpu.VMEM((TOP, TOK), jnp.int32),
            pltpu.VMEM((META, META), F32),
            pltpu.VMEM((groups, ROWS, half), BF),
            pltpu.VMEM((groups, ROWS, half), BF),
            pltpu.VMEM((groups, ROWS, half), BF),
            pltpu.VMEM((2, half, units), BF),
            pltpu.VMEM((2, half, units), BF),
            pltpu.VMEM((2, units, half), BF),
            pltpu.VMEM((groups, ROWS, half), BF),
            pltpu.VMEM((groups, ROWS, half), BF),
            pltpu.VMEM((groups, ROWS, half), BF),
            pltpu.VMEM((groups, ROWS, half), BF),
            pltpu.VMEM((NZ, TOK, half), BF),
            dma((3,)), dma((6,)),
            dma((NZ,)), dma((NZ,)),
            dma((groups, n)), dma((groups, n)),
            dma((groups, n + 1)), dma((groups, n + 1)),
            dma((groups,)), dma((groups,)),
            dma((groups, n)), dma((groups, n)),
            dma((NZ,)), dma((NZ,)),
        ],
        compiler_params=pltpu.CompilerParams(collective_id=0, has_side_effects=True, vmem_limit_bytes=60000 * 1024),
    )(tokens[0], jnp.swapaxes(expert_ids[0], 0, 1), jnp.swapaxes(gate_codes[0], 0, 1),
      gate_weight[0], up_weight[0], down_weight[0])
    return jnp.sum(parts.astype(F32), axis=0).astype(BF)[None]


def solution(mesh):
    in_specs = (
        P(None, ("dp", "expert"), "tensor"),
        P(("dp", "expert"), None, "tensor"),
        P(("dp", "expert"), None, "tensor"),
        P(("dp", "expert"), "tensor", None),
        P(None, ("dp", "expert"), None),
        P(None, ("dp", "expert"), None),
    )
    out_specs = P(None, ("dp", "expert"), "tensor")
    return jax.shard_map(local, mesh=mesh, in_specs=in_specs, out_specs=out_specs, check_vma=False)
```

```python
import jax
import jax.numpy as jnp
from jax import lax
from jax.experimental import pallas as pl
from jax.experimental.pallas import tpu as pltpu
from jax.sharding import PartitionSpec as P

MESH = pl.DeviceIdType.MESH
BF = jnp.bfloat16
F32 = jnp.float32
NX, NY, NZ = 4, 4, 8
TOK, TOP, SLOTS = 16, 8, 2
PLANE = NX * NY
META = 128
NEAR = (0, 1, 7, 2, 6)
GROUPS = ((0, 1), (7, 3), (5, 4), (6, 2))
STEPS = ("d0", "s0", "d3", "s3", "d1", "s1", "f0", "d2", "s2", "m0", "f3", "f1", "r0", "m1", "f2", "r1", "m2", "r2", "m3", "c0", "r3", "c1", "c2", "c3")
SENDS = ((1, 0), (3, 0), (0, 1), (0, 3), (1, 1), (3, 3), (1, 3), (3, 1), (2, 0), (0, 2), (2, 1), (1, 2), (2, 3), (3, 2), (2, 2))


def kernel(tok_hbm, ids_hbm, codes_hbm, wg_hbm, wu_hbm, wd_hbm, out_ref, held, ids_v, codes_v, meta, wg, wu, wd, sums, via, *refs):
    n_groups = len(GROUPS)
    packed, own, par, mine, theirs, back, came = (refs[n_groups * i:n_groups * (i + 1)] for i in range(7))
    (in_sem, w_sem, zs_sem, zr_sem, ds_sem, dr_sem, fs_sem, fr_sem,
     ps_sem, pr_sem, bs_sem, br_sem, os_sem, or_sem) = refs[7 * n_groups:]
    y = lax.axis_index("dp")
    e = lax.axis_index("expert")
    c = lax.axis_index("tensor")
    x = lax.rem(e, NX)
    z = e // NX
    half = sums.shape[2]

    def at(dx, dy, dz):
        return (lax.rem(y + dy, NY), lax.rem(z + dz, NZ) * NX + lax.rem(x + dx, NX), c)

    partner = (y, e, 1 - c)
    near = pl.multiple_of(c * half, 128)
    far = pl.multiple_of((1 - c) * half, 128)

    def remote(src, dst, ss, rs, device):
        copy = pltpu.make_async_remote_copy(
            src_ref=src, dst_ref=dst, send_sem=ss, recv_sem=rs, device_id=device, device_id_type=MESH)
        copy.start()
        sent.append(copy)
        return copy

    sent = []
    first = [
        pltpu.make_async_copy(ids_hbm, ids_v, in_sem.at[0]),
        pltpu.make_async_copy(codes_hbm, codes_v, in_sem.at[1]),
        pltpu.make_async_copy(tok_hbm, held.at[0, :, pl.ds(0, half)], in_sem.at[2]),
    ]
    for copy in first:
        copy.start()
    barrier = pltpu.get_barrier_semaphore()
    for dz in range(1, NZ):
        pl.semaphore_signal(barrier, inc=1, device_id=at(0, 0, dz), device_id_type=MESH)
    for dx, dy in SENDS:
        pl.semaphore_signal(barrier, inc=1, device_id=at(dx, dy, 0), device_id_type=MESH)
    pl.semaphore_signal(barrier, inc=1, device_id=partner, device_id_type=MESH)
    weights = [
        pltpu.make_async_copy(wg_hbm.at[pl.ds(near, half)], wg.at[0], w_sem.at[0]),
        pltpu.make_async_copy(wu_hbm.at[pl.ds(near, half)], wu.at[0], w_sem.at[1]),
        pltpu.make_async_copy(wg_hbm.at[pl.ds(far, half)], wg.at[1], w_sem.at[2]),
        pltpu.make_async_copy(wu_hbm.at[pl.ds(far, half)], wu.at[1], w_sem.at[3]),
        pltpu.make_async_copy(wd_hbm.at[:, pl.ds(far, half)], wd.at[1], w_sem.at[4]),
        pltpu.make_async_copy(wd_hbm.at[:, pl.ds(near, half)], wd.at[0], w_sem.at[5]),
    ]
    for copy in weights:
        copy.start()

    first[0].wait()
    first[1].wait()
    meta[...] = jnp.zeros_like(meta)
    codes = codes_v[...]
    high = codes // 256
    meta[0:TOP, 0:TOK] = ids_v[...].astype(F32)
    meta[TOP:2 * TOP, 0:TOK] = high.astype(F32)
    meta[2 * TOP:3 * TOP, 0:TOK] = (codes - high * 256).astype(F32)
    held[0, :, half:half + META] = jnp.transpose(meta[...])[0:TOK].astype(BF)
    first[2].wait()
    pl.semaphore_wait(barrier, PLANE + NZ - 1)

    order = [dz for group in GROUPS for dz in group]
    place = {dz: p for p, dz in enumerate(order)}
    width = half + META
    cut = 7 * 128
    arriving = {dz: [] for dz in order}
    for dz in sorted(order, key=lambda d: (min(d, NZ - d), d)):
        if dz and min(dz, NZ - dz) <= 2:
            p = place[dz]
            arriving[dz].append(remote(held.at[0], held.at[p], zs_sem.at[p], zr_sem.at[p], at(0, 0, dz)))

    def relay(dz):
        step = 1 if dz == 2 else NZ - 1
        p = place[dz]
        onward = (dz + step) % NZ
        q = place[onward]
        arriving[onward].append(remote(held.at[p], held.at[q], zs_sem.at[q], zr_sem.at[q], at(0, 0, step)))
        q = place[4]
        side = 0 if dz == 2 else 1
        part = pl.ds(0, cut) if side == 0 else pl.ds(cut, width - cut)
        arriving[4].append(remote(held.at[p, :, part], held.at[q, :, part], zs_sem.at[NZ + side], zr_sem.at[NZ + side], at(0, 0, 2 * step % NZ)))

    gates = [None] * n_groups
    d_copies = [None] * n_groups
    f_copies = [None] * n_groups
    p_copies = [None] * n_groups
    b_copies = [None] * n_groups
    o_copies = []
    passing = {2: [], NZ - 2: []}
    waited = set()

    def routes(g):
        per = len(GROUPS[g])
        block_rows = per * SLOTS
        tokens = per * TOK
        rows = PLANE * block_rows
        lane = lax.broadcasted_iota(jnp.int32, (1, rows), 1)
        offset = lane // block_rows
        slot = lax.rem(lane, block_rows)
        slot_rank = lax.rem(slot, SLOTS).astype(F32)
        slot_expert = (lax.rem(y + offset // NX, NY) * (NX * NZ) + z * NX + lax.rem(x + lax.rem(offset, NX), NX)).astype(F32)
        row = lax.broadcasted_iota(jnp.int32, (tokens, 1), 0)
        same_source = (row // TOK) == slot // SLOTS
        r_i = lax.broadcasted_iota(jnp.int32, (tokens, tokens), 0)
        c_i = lax.broadcasted_iota(jnp.int32, (tokens, tokens), 1)
        earlier = jnp.where((r_i // TOK == c_i // TOK) & (c_i < r_i), 1.0, 0.0).astype(BF)
        p = place[GROUPS[g][0]]
        m = held[p:p + per, :, half:half + META].reshape(tokens, META).astype(F32)
        number = m[:, TOP:2 * TOP] * 256.0 + m[:, 2 * TOP:3 * TOP]
        share = number / jnp.sum(number, axis=1, keepdims=True)
        hit = jnp.zeros((tokens, rows), F32)
        gate = jnp.zeros((tokens, rows), F32)
        for k in range(TOP):
            chosen = m[:, k:k + 1] == slot_expert
            hit = jnp.where(chosen, 1.0, hit)
            gate = jnp.where(chosen, share[:, k:k + 1], gate)
        rank = jnp.dot(earlier, hit.astype(BF), preferred_element_type=F32)
        take = (hit > 0.5) & same_source & (rank == slot_rank)
        return jnp.where(take, 1.0, 0.0), jnp.where(take, gate, 0.0)

    def block(g, dx, dy):
        size = len(GROUPS[g]) * SLOTS
        return pl.ds((dy * NX + dx) * size, size)

    def dispatch(g):
        per = len(GROUPS[g])
        p = place[GROUPS[g][0]]
        for dz in GROUPS[g]:
            for copy in arriving[dz]:
                copy.wait_recv()
            if dz in (2, NZ - 2):
                relay(dz)
        take, gates[g] = routes(g)
        rows = held[p:p + per, :, 0:half].reshape(per * TOK, half)
        packed[g][...] = jnp.dot(jnp.transpose(take).astype(BF), rows, preferred_element_type=F32).astype(BF)

    def send(g):
        d_copies[g] = [
            remote(packed[g].at[block(g, dx, dy)], own[g].at[block(g, dx, dy)], ds_sem.at[g, i], dr_sem.at[g, i], at(dx, dy, 0))
            for i, (dx, dy) in enumerate(SENDS)]
        own[g][block(g, 0, 0)] = packed[g][block(g, 0, 0)]

    def forward(g):
        f_copies[g] = []
        for i, (dx, dy) in enumerate(((0, 0),) + SENDS):
            if i:
                d_copies[g][i - 1].wait_recv()
            f_copies[g].append(remote(own[g].at[block(g, dx, dy)], par[g].at[block(g, dx, dy)], fs_sem.at[g, i], fr_sem.at[g, i], partner))

    def once(copies):
        for copy in copies:
            if id(copy) not in waited:
                waited.add(id(copy))
                copy.wait()

    def matmuls(g):
        once(weights[:2])
        rows = own[g][...]
        gated = jnp.dot(rows, wg[0], preferred_element_type=F32)
        lifted = jnp.dot(rows, wu[0], preferred_element_type=F32)
        for copy in f_copies[g]:
            copy.wait_recv()
        once(weights[2:])
        rows = par[g][...]
        gated += jnp.dot(rows, wg[1], preferred_element_type=F32)
        lifted += jnp.dot(rows, wu[1], preferred_element_type=F32)
        hidden = (gated / (1.0 + jnp.exp(-gated)) * lifted).astype(BF)
        mine[g][...] = jnp.dot(hidden, wd[1], preferred_element_type=F32).astype(BF)
        p_copies[g] = remote(mine[g], theirs[g], ps_sem.at[g], pr_sem.at[g], partner)
        back[g][...] = jnp.dot(hidden, wd[0], preferred_element_type=F32).astype(BF)

    def give_back(g):
        p_copies[g].wait_recv()
        back[g][...] = (back[g][...].astype(F32) + theirs[g][...].astype(F32)).astype(BF)
        b_copies[g] = [
            remote(back[g].at[block(g, dx, dy)], came[g].at[block(g, dx, dy)], bs_sem.at[g, i], br_sem.at[g, i],
                   at((NX - dx) % NX, (NY - dy) % NY, 0))
            for i, (dx, dy) in enumerate(SENDS)]
        came[g][block(g, 0, 0)] = back[g][block(g, 0, 0)]

    def combine(g):
        per = len(GROUPS[g])
        p = place[GROUPS[g][0]]
        for copy in b_copies[g]:
            copy.wait_recv()
        whole = gates[g].astype(BF)
        rest = (gates[g] - whole.astype(F32)).astype(BF)
        rows = came[g][...]
        total = jnp.dot(whole, rows, preferred_element_type=F32) + jnp.dot(rest, rows, preferred_element_type=F32)
        for q, dz in enumerate(GROUPS[g]):
            part = total[q * TOK:(q + 1) * TOK]
            k = p + q
            if dz == 0:
                out_ref[0] = part.astype(BF)
                continue
            if dz in (2, NZ - 2):
                for copy in passing[dz]:
                    copy.wait_recv()
                side = 0 if dz == 2 else 1
                part += via[side].astype(F32)
                span = pl.ds(0, cut) if side == 0 else pl.ds(cut, half - cut)
                more = via[2 + side, :, span].astype(F32)
                part = jnp.concatenate([part[:, :cut] + more, part[:, cut:]] if side == 0 else [part[:, :cut], part[:, cut:] + more], axis=1)
            sums[k] = part.astype(BF)
            if dz in NEAR:
                i = NEAR.index(dz)
                o_copies.append(remote(sums.at[k], out_ref.at[i], os_sem.at[i], or_sem.at[i], at(0, 0, NZ - dz)))
            elif dz == 4:
                for side, span, step in ((0, pl.ds(0, cut), NZ - 2), (1, pl.ds(cut, half - cut), 2)):
                    i = NZ + 2 + side
                    passing[2 if side == 0 else NZ - 2].append(
                        remote(sums.at[k, :, span], via.at[2 + side, :, span], os_sem.at[i], or_sem.at[i], at(0, 0, step)))
            else:
                side = 0 if dz == 3 else 1
                i = NZ + side
                passing[2 if side == 0 else NZ - 2].append(
                    remote(sums.at[k], via.at[side], os_sem.at[i], or_sem.at[i], at(0, 0, NZ - 1 if side == 0 else 1)))

    stages = {"d": dispatch, "s": send, "f": forward, "m": matmuls, "r": give_back, "c": combine}
    for step in STEPS:
        stages[step[0]](int(step[1]))
    for copy in o_copies:
        copy.wait_recv()
    for copy in sent:
        copy.wait_send()


def local(tokens, gate_weight, up_weight, down_weight, expert_ids, gate_codes):
    half = tokens.shape[2]
    units = gate_weight.shape[2]
    groups = len(GROUPS)
    dma = pltpu.SemaphoreType.DMA
    n = len(SENDS)
    parts = pl.pallas_call(
        kernel,
        out_shape=jax.ShapeDtypeStruct((len(NEAR), TOK, half), BF),
        in_specs=[pl.BlockSpec(memory_space=pl.ANY)] * 6,
        out_specs=pl.BlockSpec(memory_space=pltpu.VMEM),
        scratch_shapes=[
            pltpu.VMEM((NZ, TOK, half + META), BF),
            pltpu.VMEM((TOP, TOK), jnp.int32),
            pltpu.VMEM((TOP, TOK), jnp.int32),
            pltpu.VMEM((META, META), F32),
            pltpu.VMEM((2, half, units), BF),
            pltpu.VMEM((2, half, units), BF),
            pltpu.VMEM((2, units, half), BF),
            pltpu.VMEM((NZ, TOK, half), BF),
            pltpu.VMEM((4, TOK, half), BF),
            *[pltpu.VMEM((PLANE * SLOTS * len(group), half), BF) for _ in range(7) for group in GROUPS],
            dma((3,)), dma((6,)),
            dma((NZ + 2,)), dma((NZ + 2,)),
            dma((groups, n)), dma((groups, n)),
            dma((groups, n + 1)), dma((groups, n + 1)),
            dma((groups,)), dma((groups,)),
            dma((groups, n)), dma((groups, n)),
            dma((NZ + 4,)), dma((NZ + 4,)),
        ],
        compiler_params=pltpu.CompilerParams(collective_id=0, has_side_effects=True, vmem_limit_bytes=60000 * 1024),
    )(tokens[0], jnp.swapaxes(expert_ids[0], 0, 1), jnp.swapaxes(gate_codes[0], 0, 1),
      gate_weight[0], up_weight[0], down_weight[0])
    return jnp.sum(parts.astype(F32), axis=0).astype(BF)[None]


def solution(mesh):
    in_specs = (
        P(None, ("dp", "expert"), "tensor"),
        P(("dp", "expert"), None, "tensor"),
        P(("dp", "expert"), None, "tensor"),
        P(("dp", "expert"), "tensor", None),
        P(None, ("dp", "expert"), None),
        P(None, ("dp", "expert"), None),
    )
    out_specs = P(None, ("dp", "expert"), "tensor")
    return jax.shard_map(local, mesh=mesh, in_specs=in_specs, out_specs=out_specs, check_vma=False)
```

```python
import jax
import jax.numpy as jnp
from jax import lax
from jax.experimental import pallas as pl
from jax.experimental.pallas import tpu as pltpu
from jax.sharding import PartitionSpec as P

MESH = pl.DeviceIdType.MESH
BF = jnp.bfloat16
F32 = jnp.float32
NX, NY, NZ = 4, 4, 8
TOK, TOP, SLOTS = 16, 8, 2
PLANE = NX * NY
META = 128
NEAR = (0, 1, 7, 2, 6, 4)
GROUPS = ((0,), (1, 7), (6, 2), (3, 5), (4,))
MERGED = ((0, 1), (3, 4), (2,))
STEPS = ("d0", "s0", "d1", "s1", "d2", "s2", "f0", "d3", "s3", "f1", "d4", "s4", "m0", "f2", "r0", "r1", "f3", "f4", "m1", "r3", "r4", "m2", "c0", "c1", "r2", "c3", "c4", "c2", "v")
SENDS = ((1, 0), (3, 0), (0, 1), (0, 3), (1, 1), (3, 3), (1, 3), (3, 1), (2, 0), (0, 2), (2, 1), (1, 2), (2, 3), (3, 2), (2, 2))


def kernel(tok_hbm, ids_hbm, codes_hbm, wg_hbm, wu_hbm, wd_hbm, out_ref, held, ids_v, codes_v, meta, wg, wu, wd, sums, via, parts, *refs):
    n_groups = len(GROUPS)
    n_merged = len(MERGED)
    packed, own, par, mine, theirs, back, came = (refs[n_merged * i:n_merged * (i + 1)] for i in range(7))
    (in_sem, w_sem, zs_sem, zr_sem, ds_sem, dr_sem, fs_sem, fr_sem,
     ps_sem, pr_sem, bs_sem, br_sem, os_sem, or_sem) = refs[7 * n_merged:]
    y = lax.axis_index("dp")
    e = lax.axis_index("expert")
    c = lax.axis_index("tensor")
    x = lax.rem(e, NX)
    z = e // NX
    half = sums.shape[2]

    def at(dx, dy, dz):
        return (lax.rem(y + dy, NY), lax.rem(z + dz, NZ) * NX + lax.rem(x + dx, NX), c)

    partner = (y, e, 1 - c)
    near = pl.multiple_of(c * half, 128)
    far = pl.multiple_of((1 - c) * half, 128)

    def remote(src, dst, ss, rs, device):
        copy = pltpu.make_async_remote_copy(
            src_ref=src, dst_ref=dst, send_sem=ss, recv_sem=rs, device_id=device, device_id_type=MESH)
        copy.start()
        sent.append(copy)
        return copy

    sent = []
    first = [
        pltpu.make_async_copy(ids_hbm, ids_v, in_sem.at[0]),
        pltpu.make_async_copy(codes_hbm, codes_v, in_sem.at[1]),
        pltpu.make_async_copy(tok_hbm, held.at[0, :, pl.ds(0, half)], in_sem.at[2]),
    ]
    for copy in first:
        copy.start()
    barrier = pltpu.get_barrier_semaphore()
    for dz in range(1, NZ):
        pl.semaphore_signal(barrier, inc=1, device_id=at(0, 0, dz), device_id_type=MESH)
    for dx, dy in SENDS:
        pl.semaphore_signal(barrier, inc=1, device_id=at(dx, dy, 0), device_id_type=MESH)
    pl.semaphore_signal(barrier, inc=1, device_id=partner, device_id_type=MESH)
    weights = [
        pltpu.make_async_copy(wg_hbm.at[pl.ds(near, half)], wg.at[0], w_sem.at[0]),
        pltpu.make_async_copy(wu_hbm.at[pl.ds(near, half)], wu.at[0], w_sem.at[1]),
        pltpu.make_async_copy(wg_hbm.at[pl.ds(far, half)], wg.at[1], w_sem.at[2]),
        pltpu.make_async_copy(wu_hbm.at[pl.ds(far, half)], wu.at[1], w_sem.at[3]),
        pltpu.make_async_copy(wd_hbm.at[:, pl.ds(far, half)], wd.at[1], w_sem.at[4]),
        pltpu.make_async_copy(wd_hbm.at[:, pl.ds(near, half)], wd.at[0], w_sem.at[5]),
    ]
    for copy in weights:
        copy.start()

    first[0].wait()
    first[1].wait()
    meta[...] = jnp.zeros_like(meta)
    codes = codes_v[...]
    high = codes // 256
    meta[0:TOP, 0:TOK] = ids_v[...].astype(F32)
    meta[TOP:2 * TOP, 0:TOK] = high.astype(F32)
    meta[2 * TOP:3 * TOP, 0:TOK] = (codes - high * 256).astype(F32)
    held[0, :, half:half + META] = jnp.transpose(meta[...])[0:TOK].astype(BF)
    first[2].wait()
    pl.semaphore_wait(barrier, PLANE + NZ - 1)

    order = [dz for group in GROUPS for dz in group]
    place = {dz: p for p, dz in enumerate(order)}
    width = half + META
    cut = 7 * 128
    arriving = {dz: [] for dz in order}
    for dz in sorted(order, key=lambda d: (min(d, NZ - d), d)):
        if dz and min(dz, NZ - dz) <= 2:
            p = place[dz]
            arriving[dz].append(remote(held.at[0], held.at[p], zs_sem.at[p], zr_sem.at[p], at(0, 0, dz)))

    def relay(dz):
        step = 1 if dz == 2 else NZ - 1
        p = place[dz]
        onward = (dz + step) % NZ
        q = place[onward]
        arriving[onward].append(remote(held.at[p], held.at[q], zs_sem.at[q], zr_sem.at[q], at(0, 0, step)))
        q = place[4]
        side = 0 if dz == 2 else 1
        part = pl.ds(0, cut) if side == 0 else pl.ds(cut, width - cut)
        arriving[4].append(remote(held.at[p, :, part], held.at[q, :, part], zs_sem.at[NZ + side], zr_sem.at[NZ + side], at(0, 0, 2 * step % NZ)))

    gates = [None] * n_groups
    d_copies = [None] * n_groups
    f_copies = [None] * n_groups
    p_copies = [None] * n_groups
    b_copies = [None] * n_groups
    o_copies = []
    passing = {2: [], NZ - 2: []}
    later = {}
    waited = set()

    def routes(g):
        per = len(GROUPS[g])
        block_rows = per * SLOTS
        tokens = per * TOK
        rows = PLANE * block_rows
        lane = lax.broadcasted_iota(jnp.int32, (1, rows), 1)
        offset = lane // block_rows
        slot = lax.rem(lane, block_rows)
        slot_rank = lax.rem(slot, SLOTS).astype(F32)
        slot_expert = (lax.rem(y + offset // NX, NY) * (NX * NZ) + z * NX + lax.rem(x + lax.rem(offset, NX), NX)).astype(F32)
        row = lax.broadcasted_iota(jnp.int32, (tokens, 1), 0)
        same_source = (row // TOK) == slot // SLOTS
        r_i = lax.broadcasted_iota(jnp.int32, (tokens, tokens), 0)
        c_i = lax.broadcasted_iota(jnp.int32, (tokens, tokens), 1)
        earlier = jnp.where((r_i // TOK == c_i // TOK) & (c_i < r_i), 1.0, 0.0).astype(BF)
        p = place[GROUPS[g][0]]
        m = held[p:p + per, :, half:half + META].reshape(tokens, META).astype(F32)
        number = m[:, TOP:2 * TOP] * 256.0 + m[:, 2 * TOP:3 * TOP]
        share = number / jnp.sum(number, axis=1, keepdims=True)
        hit = jnp.zeros((tokens, rows), F32)
        gate = jnp.zeros((tokens, rows), F32)
        for k in range(TOP):
            chosen = m[:, k:k + 1] == slot_expert
            hit = jnp.where(chosen, 1.0, hit)
            gate = jnp.where(chosen, share[:, k:k + 1], gate)
        rank = jnp.dot(earlier, hit.astype(BF), preferred_element_type=F32)
        take = (hit > 0.5) & same_source & (rank == slot_rank)
        return jnp.where(take, 1.0, 0.0), jnp.where(take, gate, 0.0)

    home, start = {}, {}
    for k, members in enumerate(MERGED):
        for q, g in enumerate(members):
            home[g] = k
            start[g] = sum(len(GROUPS[h]) for h in members[:q]) * SLOTS * PLANE

    def block(g, dx, dy):
        size = len(GROUPS[g]) * SLOTS
        return pl.ds(start[g] + (dy * NX + dx) * size, size)

    def rows_of(g):
        return pl.ds(start[g], len(GROUPS[g]) * SLOTS * PLANE)

    def dispatch(g):
        per = len(GROUPS[g])
        p = place[GROUPS[g][0]]
        for dz in GROUPS[g]:
            for copy in arriving[dz]:
                copy.wait_recv()
            if dz in (2, NZ - 2):
                relay(dz)
        take, gates[g] = routes(g)
        rows = held[p:p + per, :, 0:half].reshape(per * TOK, half)
        packed[home[g]][rows_of(g)] = jnp.dot(jnp.transpose(take).astype(BF), rows, preferred_element_type=F32).astype(BF)

    def send(g):
        d_copies[g] = [
            remote(packed[home[g]].at[block(g, dx, dy)], own[home[g]].at[block(g, dx, dy)], ds_sem.at[g, i], dr_sem.at[g, i], at(dx, dy, 0))
            for i, (dx, dy) in enumerate(SENDS)]
        own[home[g]][block(g, 0, 0)] = packed[home[g]][block(g, 0, 0)]

    def forward(g):
        f_copies[g] = []
        for i, (dx, dy) in enumerate(((0, 0),) + SENDS):
            if i:
                d_copies[g][i - 1].wait_recv()
            f_copies[g].append(remote(own[home[g]].at[block(g, dx, dy)], par[home[g]].at[block(g, dx, dy)], fs_sem.at[g, i], fr_sem.at[g, i], partner))

    def once(copies):
        for copy in copies:
            if id(copy) not in waited:
                waited.add(id(copy))
                copy.wait()

    def matmuls(m):
        once(weights[:2])
        rows = own[m][...]
        gated = jnp.dot(rows, wg[0], preferred_element_type=F32)
        lifted = jnp.dot(rows, wu[0], preferred_element_type=F32)
        for g in MERGED[m]:
            for copy in f_copies[g]:
                copy.wait_recv()
        once(weights[2:])
        rows = par[m][...]
        gated += jnp.dot(rows, wg[1], preferred_element_type=F32)
        lifted += jnp.dot(rows, wu[1], preferred_element_type=F32)
        hidden = (gated / (1.0 + jnp.exp(-gated)) * lifted).astype(BF)
        mine[m][...] = jnp.dot(hidden, wd[1], preferred_element_type=F32).astype(BF)
        p_copies[m] = remote(mine[m], theirs[m], ps_sem.at[m], pr_sem.at[m], partner)
        back[m][...] = jnp.dot(hidden, wd[0], preferred_element_type=F32).astype(BF)

    def give_back(g):
        m = home[g]
        if g == MERGED[m][0]:
            p_copies[m].wait_recv()
        rows = rows_of(g)
        back[m][rows] = (back[m][rows].astype(F32) + theirs[m][rows].astype(F32)).astype(BF)
        b_copies[g] = [
            remote(back[m].at[block(g, dx, dy)], came[m].at[block(g, dx, dy)], bs_sem.at[g, i], br_sem.at[g, i],
                   at((NX - dx) % NX, (NY - dy) % NY, 0))
            for i, (dx, dy) in enumerate(SENDS)]
        came[m][block(g, 0, 0)] = back[m][block(g, 0, 0)]

    def combine(g):
        per = len(GROUPS[g])
        p = place[GROUPS[g][0]]
        for copy in b_copies[g]:
            copy.wait_recv()
        whole = gates[g].astype(BF)
        rest = (gates[g] - whole.astype(F32)).astype(BF)
        rows = came[home[g]][rows_of(g)]
        total = jnp.dot(whole, rows, preferred_element_type=F32) + jnp.dot(rest, rows, preferred_element_type=F32)
        for q, dz in enumerate(GROUPS[g]):
            part = total[q * TOK:(q + 1) * TOK]
            if dz == 0:
                parts[0] = part.astype(BF)
            elif dz in passing:
                later[dz] = part
            elif dz in NEAR:
                home_bound(dz, part)
            else:
                onward = 2 if dz == 3 else NZ - 2
                side = 0 if dz == 3 else 1
                i = NZ + side
                sums[p + q] = part.astype(BF)
                passing[onward].append(
                    remote(sums.at[p + q], via.at[side], os_sem.at[i], or_sem.at[i], at(0, 0, NZ - 1 if side == 0 else 1)))

    def home_bound(dz, part):
        i, k = NEAR.index(dz), place[dz]
        sums[k] = part.astype(BF)
        o_copies.append(remote(sums.at[k], parts.at[i], os_sem.at[i], or_sem.at[i], at(0, 0, NZ - dz)))

    def hand_on():
        for side, dz in enumerate(passing):
            for copy in passing[dz]:
                copy.wait_recv()
            home_bound(dz, later[dz] + via[side].astype(F32))

    stages = {"d": dispatch, "s": send, "f": forward, "m": matmuls, "r": give_back, "c": combine}
    for step in STEPS:
        if step == "v":
            hand_on()
        else:
            stages[step[0]](int(step[1]))
    for copy in o_copies:
        copy.wait_recv()
    total = parts[0].astype(F32)
    for i in range(1, len(NEAR)):
        total += parts[i].astype(F32)
    out_ref[0] = total.astype(BF)
    for copy in sent:
        copy.wait_send()


def local(tokens, gate_weight, up_weight, down_weight, expert_ids, gate_codes):
    half = tokens.shape[2]
    units = gate_weight.shape[2]
    groups = len(GROUPS)
    dma = pltpu.SemaphoreType.DMA
    n = len(SENDS)
    mixed = pl.pallas_call(
        kernel,
        out_shape=jax.ShapeDtypeStruct((1, TOK, half), BF),
        in_specs=[pl.BlockSpec(memory_space=pl.ANY)] * 6,
        out_specs=pl.BlockSpec(memory_space=pltpu.VMEM),
        scratch_shapes=[
            pltpu.VMEM((NZ, TOK, half + META), BF),
            pltpu.VMEM((TOP, TOK), jnp.int32),
            pltpu.VMEM((TOP, TOK), jnp.int32),
            pltpu.VMEM((META, META), F32),
            pltpu.VMEM((2, half, units), BF),
            pltpu.VMEM((2, half, units), BF),
            pltpu.VMEM((2, units, half), BF),
            pltpu.VMEM((NZ, TOK, half), BF),
            pltpu.VMEM((2, TOK, half), BF),
            pltpu.VMEM((len(NEAR), TOK, half), BF),
            *[pltpu.VMEM((PLANE * SLOTS * sum(len(GROUPS[g]) for g in members), half), BF) for _ in range(7) for members in MERGED],
            dma((3,)), dma((6,)),
            dma((NZ + 2,)), dma((NZ + 2,)),
            dma((groups, n)), dma((groups, n)),
            dma((groups, n + 1)), dma((groups, n + 1)),
            dma((groups,)), dma((groups,)),
            dma((groups, n)), dma((groups, n)),
            dma((NZ + 2,)), dma((NZ + 2,)),
        ],
        compiler_params=pltpu.CompilerParams(collective_id=0, has_side_effects=True, vmem_limit_bytes=60000 * 1024),
    )(tokens[0], jnp.swapaxes(expert_ids[0], 0, 1), jnp.swapaxes(gate_codes[0], 0, 1),
      gate_weight[0], up_weight[0], down_weight[0])
    return mixed


def solution(mesh):
    in_specs = (
        P(None, ("dp", "expert"), "tensor"),
        P(("dp", "expert"), None, "tensor"),
        P(("dp", "expert"), None, "tensor"),
        P(("dp", "expert"), "tensor", None),
        P(None, ("dp", "expert"), None),
        P(None, ("dp", "expert"), None),
    )
    out_specs = P(None, ("dp", "expert"), "tensor")
    return jax.shard_map(local, mesh=mesh, in_specs=in_specs, out_specs=out_specs, check_vma=False)
```

```python
import jax
import jax.numpy as jnp
from jax import lax
from jax.experimental import pallas as pl
from jax.experimental.pallas import tpu as pltpu
from jax.sharding import PartitionSpec as P

MESH = pl.DeviceIdType.MESH
BF = jnp.bfloat16
F32 = jnp.float32
NX, NY, NZ = 4, 4, 8
TOK, TOP, SLOTS = 16, 8, 2
PLANE = NX * NY
META = 128
NEAR = (0, 1, 7, 2, 6, 4)
GROUPS = ((0,), (1, 7), (6, 2), (3, 5), (4,))
MERGED = ((0, 1), (3, 4), (2,))
STEPS = ("d0", "s0", "d1", "s1", "d2", "s2", "f0", "d3", "s3", "f1", "d4", "s4", "m0", "f2", "r0", "r1", "f3", "f4", "m1", "r3", "r4", "c0", "m2", "r2", "c1", "c3", "c4", "c2", "v")
SENDS = ((2, 2), (3, 2), (2, 3), (1, 2), (2, 1), (0, 2), (2, 0), (3, 1), (1, 3), (3, 3), (1, 1), (0, 3), (0, 1), (3, 0), (1, 0))


def kernel(tok_hbm, ids_hbm, codes_hbm, wg_hbm, wu_hbm, wd_hbm, out_ref, held, ids_v, codes_v, meta, wg, wu, wd, sums, via, parts, *refs):
    n_groups = len(GROUPS)
    n_merged = len(MERGED)
    packed, own, par, mine, theirs, back, came = (refs[n_merged * i:n_merged * (i + 1)] for i in range(7))
    (in_sem, w_sem, zs_sem, zr_sem, ds_sem, dr_sem, fs_sem, fr_sem,
     ps_sem, pr_sem, bs_sem, br_sem, os_sem, or_sem) = refs[7 * n_merged:]
    y = lax.axis_index("dp")
    e = lax.axis_index("expert")
    c = lax.axis_index("tensor")
    x = lax.rem(e, NX)
    z = e // NX
    half = sums.shape[2]

    def at(dx, dy, dz):
        return (lax.rem(y + dy, NY), lax.rem(z + dz, NZ) * NX + lax.rem(x + dx, NX), c)

    partner = (y, e, 1 - c)
    near = pl.multiple_of(c * half, 128)
    far = pl.multiple_of((1 - c) * half, 128)

    def remote(src, dst, ss, rs, device):
        copy = pltpu.make_async_remote_copy(
            src_ref=src, dst_ref=dst, send_sem=ss, recv_sem=rs, device_id=device, device_id_type=MESH)
        copy.start()
        sent.append(copy)
        return copy

    sent = []
    first = [
        pltpu.make_async_copy(ids_hbm, ids_v, in_sem.at[0]),
        pltpu.make_async_copy(codes_hbm, codes_v, in_sem.at[1]),
        pltpu.make_async_copy(tok_hbm, held.at[0, :, pl.ds(0, half)], in_sem.at[2]),
    ]
    for copy in first:
        copy.start()
    barrier = pltpu.get_barrier_semaphore()
    for dz in range(1, NZ):
        pl.semaphore_signal(barrier, inc=1, device_id=at(0, 0, dz), device_id_type=MESH)
    for dx, dy in SENDS:
        pl.semaphore_signal(barrier, inc=1, device_id=at(dx, dy, 0), device_id_type=MESH)
    pl.semaphore_signal(barrier, inc=1, device_id=partner, device_id_type=MESH)
    weights = [
        pltpu.make_async_copy(wg_hbm.at[pl.ds(near, half)], wg.at[0], w_sem.at[0]),
        pltpu.make_async_copy(wu_hbm.at[pl.ds(near, half)], wu.at[0], w_sem.at[1]),
        pltpu.make_async_copy(wg_hbm.at[pl.ds(far, half)], wg.at[1], w_sem.at[2]),
        pltpu.make_async_copy(wu_hbm.at[pl.ds(far, half)], wu.at[1], w_sem.at[3]),
        pltpu.make_async_copy(wd_hbm.at[:, pl.ds(far, half)], wd.at[1], w_sem.at[4]),
        pltpu.make_async_copy(wd_hbm.at[:, pl.ds(near, half)], wd.at[0], w_sem.at[5]),
    ]
    for copy in weights:
        copy.start()

    first[0].wait()
    first[1].wait()
    meta[...] = jnp.zeros_like(meta)
    codes = codes_v[...]
    high = codes // 256
    meta[0:TOP, 0:TOK] = ids_v[...].astype(F32)
    meta[TOP:2 * TOP, 0:TOK] = high.astype(F32)
    meta[2 * TOP:3 * TOP, 0:TOK] = (codes - high * 256).astype(F32)
    held[0, :, half:half + META] = jnp.transpose(meta[...])[0:TOK].astype(BF)
    first[2].wait()
    pl.semaphore_wait(barrier, PLANE + NZ - 1)

    order = [dz for group in GROUPS for dz in group]
    place = {dz: p for p, dz in enumerate(order)}
    width = half + META
    cut = 7 * 128
    arriving = {dz: [] for dz in order}
    for dz in sorted(order, key=lambda d: (min(d, NZ - d), d)):
        if dz and min(dz, NZ - dz) <= 2:
            p = place[dz]
            arriving[dz].append(remote(held.at[0], held.at[p], zs_sem.at[p], zr_sem.at[p], at(0, 0, dz)))

    def relay(dz):
        step = 1 if dz == 2 else NZ - 1
        p = place[dz]
        onward = (dz + step) % NZ
        q = place[onward]
        arriving[onward].append(remote(held.at[p], held.at[q], zs_sem.at[q], zr_sem.at[q], at(0, 0, step)))
        q = place[4]
        side = 0 if dz == 2 else 1
        part = pl.ds(0, cut) if side == 0 else pl.ds(cut, width - cut)
        arriving[4].append(remote(held.at[p, :, part], held.at[q, :, part], zs_sem.at[NZ + side], zr_sem.at[NZ + side], at(0, 0, 2 * step % NZ)))

    gates = [None] * n_groups
    d_copies = [None] * n_groups
    f_copies = [None] * n_groups
    p_copies = [None] * n_groups
    b_copies = [None] * n_groups
    o_copies = []
    passing = {2: [], NZ - 2: []}
    later = {}
    waited = set()

    def routes(g):
        per = len(GROUPS[g])
        block_rows = per * SLOTS
        tokens = per * TOK
        rows = PLANE * block_rows
        lane = lax.broadcasted_iota(jnp.int32, (1, rows), 1)
        offset = lane // block_rows
        slot = lax.rem(lane, block_rows)
        slot_rank = lax.rem(slot, SLOTS).astype(F32)
        slot_expert = (lax.rem(y + offset // NX, NY) * (NX * NZ) + z * NX + lax.rem(x + lax.rem(offset, NX), NX)).astype(F32)
        row = lax.broadcasted_iota(jnp.int32, (tokens, 1), 0)
        same_source = (row // TOK) == slot // SLOTS
        r_i = lax.broadcasted_iota(jnp.int32, (tokens, tokens), 0)
        c_i = lax.broadcasted_iota(jnp.int32, (tokens, tokens), 1)
        earlier = jnp.where((r_i // TOK == c_i // TOK) & (c_i < r_i), 1.0, 0.0).astype(BF)
        p = place[GROUPS[g][0]]
        m = held[p:p + per, :, half:half + META].reshape(tokens, META).astype(F32)
        number = m[:, TOP:2 * TOP] * 256.0 + m[:, 2 * TOP:3 * TOP]
        share = number / jnp.sum(number, axis=1, keepdims=True)
        hit = jnp.zeros((tokens, rows), F32)
        gate = jnp.zeros((tokens, rows), F32)
        for k in range(TOP):
            chosen = m[:, k:k + 1] == slot_expert
            hit = jnp.where(chosen, 1.0, hit)
            gate = jnp.where(chosen, share[:, k:k + 1], gate)
        rank = jnp.dot(earlier, hit.astype(BF), preferred_element_type=F32)
        take = (hit > 0.5) & same_source & (rank == slot_rank)
        return jnp.where(take, 1.0, 0.0), jnp.where(take, gate, 0.0)

    home, start = {}, {}
    for k, members in enumerate(MERGED):
        for q, g in enumerate(members):
            home[g] = k
            start[g] = sum(len(GROUPS[h]) for h in members[:q]) * SLOTS * PLANE

    def block(g, dx, dy):
        size = len(GROUPS[g]) * SLOTS
        return pl.ds(start[g] + (dy * NX + dx) * size, size)

    def rows_of(g):
        return pl.ds(start[g], len(GROUPS[g]) * SLOTS * PLANE)

    def dispatch(g):
        per = len(GROUPS[g])
        p = place[GROUPS[g][0]]
        for dz in GROUPS[g]:
            for copy in arriving[dz]:
                copy.wait_recv()
            if dz in (2, NZ - 2):
                relay(dz)
        take, gates[g] = routes(g)
        rows = held[p:p + per, :, 0:half].reshape(per * TOK, half)
        packed[home[g]][rows_of(g)] = jnp.dot(jnp.transpose(take).astype(BF), rows, preferred_element_type=F32).astype(BF)

    def send(g):
        d_copies[g] = [
            remote(packed[home[g]].at[block(g, dx, dy)], own[home[g]].at[block(g, dx, dy)], ds_sem.at[g, i], dr_sem.at[g, i], at(dx, dy, 0))
            for i, (dx, dy) in enumerate(SENDS)]
        own[home[g]][block(g, 0, 0)] = packed[home[g]][block(g, 0, 0)]

    def forward(g):
        f_copies[g] = []
        for i, (dx, dy) in enumerate(((0, 0),) + SENDS):
            if i:
                d_copies[g][i - 1].wait_recv()
            f_copies[g].append(remote(own[home[g]].at[block(g, dx, dy)], par[home[g]].at[block(g, dx, dy)], fs_sem.at[g, i], fr_sem.at[g, i], partner))

    def once(copies):
        for copy in copies:
            if id(copy) not in waited:
                waited.add(id(copy))
                copy.wait()

    def matmuls(m):
        once(weights[:2])
        rows = own[m][...]
        gated = jnp.dot(rows, wg[0], preferred_element_type=F32)
        lifted = jnp.dot(rows, wu[0], preferred_element_type=F32)
        for g in MERGED[m]:
            for copy in f_copies[g]:
                copy.wait_recv()
        once(weights[2:])
        rows = par[m][...]
        gated += jnp.dot(rows, wg[1], preferred_element_type=F32)
        lifted += jnp.dot(rows, wu[1], preferred_element_type=F32)
        hidden = (gated / (1.0 + jnp.exp(-gated)) * lifted).astype(BF)
        mine[m][...] = jnp.dot(hidden, wd[1], preferred_element_type=F32).astype(BF)
        p_copies[m] = remote(mine[m], theirs[m], ps_sem.at[m], pr_sem.at[m], partner)
        back[m][...] = jnp.dot(hidden, wd[0], preferred_element_type=F32).astype(BF)

    def give_back(g):
        m = home[g]
        if g == MERGED[m][0]:
            p_copies[m].wait_recv()
        rows = rows_of(g)
        back[m][rows] = (back[m][rows].astype(F32) + theirs[m][rows].astype(F32)).astype(BF)
        b_copies[g] = [
            remote(back[m].at[block(g, dx, dy)], came[m].at[block(g, dx, dy)], bs_sem.at[g, i], br_sem.at[g, i],
                   at((NX - dx) % NX, (NY - dy) % NY, 0))
            for i, (dx, dy) in enumerate(SENDS)]
        came[m][block(g, 0, 0)] = back[m][block(g, 0, 0)]

    def combine(g):
        per = len(GROUPS[g])
        p = place[GROUPS[g][0]]
        for copy in b_copies[g]:
            copy.wait_recv()
        whole = gates[g].astype(BF)
        rest = (gates[g] - whole.astype(F32)).astype(BF)
        rows = came[home[g]][rows_of(g)]
        total = jnp.dot(whole, rows, preferred_element_type=F32) + jnp.dot(rest, rows, preferred_element_type=F32)
        for q, dz in enumerate(GROUPS[g]):
            part = total[q * TOK:(q + 1) * TOK]
            if dz == 0:
                parts[0] = part.astype(BF)
            elif dz in passing:
                later[dz] = part
            elif dz in NEAR:
                home_bound(dz, part)
            else:
                onward = 2 if dz == 3 else NZ - 2
                side = 0 if dz == 3 else 1
                i = NZ + side
                sums[p + q] = part.astype(BF)
                passing[onward].append(
                    remote(sums.at[p + q], via.at[side], os_sem.at[i], or_sem.at[i], at(0, 0, NZ - 1 if side == 0 else 1)))

    def home_bound(dz, part):
        i, k = NEAR.index(dz), place[dz]
        sums[k] = part.astype(BF)
        o_copies.append(remote(sums.at[k], parts.at[i], os_sem.at[i], or_sem.at[i], at(0, 0, NZ - dz)))

    def hand_on():
        for side, dz in enumerate(passing):
            for copy in passing[dz]:
                copy.wait_recv()
            home_bound(dz, later[dz] + via[side].astype(F32))

    stages = {"d": dispatch, "s": send, "f": forward, "m": matmuls, "r": give_back, "c": combine}
    for step in STEPS:
        if step == "v":
            hand_on()
        else:
            stages[step[0]](int(step[1]))
    for copy in o_copies:
        copy.wait_recv()
    total = parts[0].astype(F32)
    for i in range(1, len(NEAR)):
        total += parts[i].astype(F32)
    out_ref[0] = total.astype(BF)
    for copy in sent:
        copy.wait_send()


def local(tokens, gate_weight, up_weight, down_weight, expert_ids, gate_codes):
    half = tokens.shape[2]
    units = gate_weight.shape[2]
    groups = len(GROUPS)
    dma = pltpu.SemaphoreType.DMA
    n = len(SENDS)
    mixed = pl.pallas_call(
        kernel,
        out_shape=jax.ShapeDtypeStruct((1, TOK, half), BF),
        in_specs=[pl.BlockSpec(memory_space=pl.ANY)] * 6,
        out_specs=pl.BlockSpec(memory_space=pltpu.VMEM),
        scratch_shapes=[
            pltpu.VMEM((NZ, TOK, half + META), BF),
            pltpu.VMEM((TOP, TOK), jnp.int32),
            pltpu.VMEM((TOP, TOK), jnp.int32),
            pltpu.VMEM((META, META), F32),
            pltpu.VMEM((2, half, units), BF),
            pltpu.VMEM((2, half, units), BF),
            pltpu.VMEM((2, units, half), BF),
            pltpu.VMEM((NZ, TOK, half), BF),
            pltpu.VMEM((2, TOK, half), BF),
            pltpu.VMEM((len(NEAR), TOK, half), BF),
            *[pltpu.VMEM((PLANE * SLOTS * sum(len(GROUPS[g]) for g in members), half), BF) for _ in range(7) for members in MERGED],
            dma((3,)), dma((6,)),
            dma((NZ + 2,)), dma((NZ + 2,)),
            dma((groups, n)), dma((groups, n)),
            dma((groups, n + 1)), dma((groups, n + 1)),
            dma((groups,)), dma((groups,)),
            dma((groups, n)), dma((groups, n)),
            dma((NZ + 2,)), dma((NZ + 2,)),
        ],
        compiler_params=pltpu.CompilerParams(collective_id=0, has_side_effects=True, vmem_limit_bytes=60000 * 1024),
    )(tokens[0], jnp.swapaxes(expert_ids[0], 0, 1), jnp.swapaxes(gate_codes[0], 0, 1),
      gate_weight[0], up_weight[0], down_weight[0])
    return mixed


def solution(mesh):
    in_specs = (
        P(None, ("dp", "expert"), "tensor"),
        P(("dp", "expert"), None, "tensor"),
        P(("dp", "expert"), None, "tensor"),
        P(("dp", "expert"), "tensor", None),
        P(None, ("dp", "expert"), None),
        P(None, ("dp", "expert"), None),
    )
    out_specs = P(None, ("dp", "expert"), "tensor")
    return jax.shard_map(local, mesh=mesh, in_specs=in_specs, out_specs=out_specs, check_vma=False)
```
